32 devices in a mesh: pole: 4 (over y, core), dom: 8 (over z, x).
Axes of the slice: x: 2, y: 2, z: 4, core: 2. Of those that a mesh axis runs over, the one named last changes fastest.
Arguments:
- initial_block: bfloat16 [8, 8, 512, 256], P('dom'), may hold values from -24 to 24
- coupling: bfloat16 [8, 8, 512, 512], P('dom'), may hold values from -0.125 to 0.125
- pivots: bfloat16 [4, 8, 8, 2, 512, 512], P('pole', 'dom'), may hold values from -0.125 to 0.125
- interface: bfloat16 [4, 8, 3, 2, 512, 512], P('pole', 'dom'), may hold values from -0.1875 to 0.1875
- pole_values: float32 [4, 4], P('pole'), may hold values from 0.5 to 1.5
Outputs:
- filtered_basis: float32 [8, 8, 512, 256], P('dom', 'pole')
- rayleigh: float32 [256, 256], replicated
The draws below stay inside these ranges and needn't reach their ends.
All inputs are finite; a program needn't handle non-finite values.
Results may differ from the reference program's by a relative error of at most 0.008.
Values sent between devices are 32-bit elements; how exact they have to be, the bound alone decides.
No kernel may reach another device: no remote copies, remote signals or barrier semaphores. Data moves between devices by JAX's collectives and lax.ppermute only.
A program may use at most 192 MiB of HBM per device.

```python
import math
import jax
import jax.numpy as jnp
from jax import lax

B = 512
M = 256
PB = 8
PARTS_SIZE = 8
POLES = 4
ROWS = 32768


def draw_initial_block(key, part):
    noise_key = jax.random.fold_in(key, 11)
    scale_key = jax.random.fold_in(key, 23)
    base = jnp.clip(jax.random.normal(noise_key, (PARTS_SIZE, PB, B, M), jnp.float32), -6.0, 6.0)
    scales = jnp.exp(jax.random.uniform(scale_key, (PARTS_SIZE, PB, 1, 1), jnp.float32, 0.0, math.log(4.0)))
    return (base * scales).astype(jnp.bfloat16)


def shard_levels(own_key, dims, pieces, low, largest):
    factor_of, own = 1.0, jax.random.fold_in(own_key, 6)
    for axis_at, parts in pieces:
        steps = jnp.exp(jax.random.uniform(jax.random.fold_in(own, axis_at), (parts,), jnp.float32, low / len(pieces), largest / len(pieces)))
        factor_of = factor_of * jnp.repeat(steps, dims[axis_at] // parts).reshape([-1 if axis == axis_at else 1 for axis in range(len(dims))])
    return factor_of


def noise(key, extent, deviation, reach, cuts=(), kind=jnp.bfloat16):
    level = shard_levels(key, extent, cuts, -0.22, 0.18) if cuts else 1.0
    values = jax.random.normal(key, extent, jnp.float32) * deviation * level
    return jnp.minimum(jnp.maximum(values, -reach), reach).astype(kind)


def setup_inputs(seed: int = 0) -> dict:
    key_list = jax.random.split(jax.random.key(seed), 6)
    initial_block = draw_initial_block(jax.random.fold_in(key_list[5], 71), 0)
    coupling = noise(key_list[1], (PARTS_SIZE, PB, B, B), (4 * B) ** -0.5, 0.125, ((0, 8),))
    pivots = noise(key_list[2], (POLES, PARTS_SIZE, PB, 2, B, B), (4 * B) ** -0.5, 0.125, ((0, 4), (1, 8)))
    interface = noise(key_list[3], (POLES, PARTS_SIZE, 3, 2, B, B), (2 * B) ** -0.5, 0.1875, ((0, 4), (1, 8)))
    pole_values = jnp.clip(0.5 + 1.0 * jax.random.uniform(key_list[4], (POLES, 4), jnp.float32) ** shard_levels(key_list[4], (POLES, 4), ((0, 4),), -0.2, 0.2), 0.5, 1.5)
    return dict(initial_block=initial_block, coupling=coupling, pivots=pivots, interface=interface, pole_values=pole_values)


def lower_solve(factor, right_side):
    return lax.linalg.triangular_solve(factor, right_side, left_side=True, lower=True)

def complex_product(matrix, vectors):
    block_order = matrix.shape[1]
    half_width = vectors.shape[1] // 2
    stacked = matrix.reshape(2 * block_order, block_order)
    stacked_out = jnp.dot(stacked.astype(jnp.float32), vectors.astype(jnp.bfloat16).astype(jnp.float32), preferred_element_type=jnp.float32)
    real_part = stacked_out[:block_order, :half_width] - stacked_out[block_order:, half_width:]
    imag_part = stacked_out[:block_order, half_width:] + stacked_out[block_order:, :half_width]
    return jnp.concatenate([real_part, imag_part], axis=1)

def real_product(matrix, vectors):
    return jnp.dot(matrix.astype(jnp.float32), vectors.astype(jnp.bfloat16).astype(jnp.float32), preferred_element_type=jnp.float32)

def transposed_product(matrix, vectors):
    return lax.dot_general(matrix.astype(jnp.float32), vectors.astype(jnp.bfloat16).astype(jnp.float32), (((0,), (0,)), ((), ())), preferred_element_type=jnp.float32)

def inner_products(left, right_side):
    return lax.dot_general(left.astype(jnp.float32), right_side.astype(jnp.float32), (((0,), (0,)), ((), ())), precision=lax.Precision.HIGHEST, preferred_element_type=jnp.float32)

def partition_solve(inverse, coupled, source):
    previous = jnp.roll(coupled, 1, axis=0)
    initial = jnp.zeros(source.shape[1:], jnp.float32)

    def forward_step(carried, members):
        block_inverse, given, couple_prev = members
        result = complex_product(block_inverse, given + transposed_product(couple_prev, carried))
        return (result, result)
    unused, forward = lax.scan(forward_step, initial, (inverse, source, previous))

    def backward_step(carried, members):
        block_inverse, partial_value, couple_next = members
        result = partial_value + complex_product(block_inverse, real_product(couple_next, carried))
        return (result, result)
    unused, backward = lax.scan(backward_step, initial, (inverse, forward, coupled), reverse=True)
    return backward

def reference(initial_block, coupling, pivots, interface, pole_values):
    real_start = initial_block.astype(jnp.float32)
    source = jnp.concatenate([real_start, jnp.zeros_like(real_start)], axis=-1)
    basis_sum = jnp.zeros(real_start.shape, jnp.float32)
    shifted_sum = jnp.zeros(real_start.shape, jnp.float32)
    links = coupling[:, PB - 1]
    for pole_index in range(POLES):
        inverse = pivots[pole_index]
        first = jax.vmap(partition_solve)(inverse, coupling, source)
        bottom = first[:, PB - 1]
        top = first[:, 0]
        top_next = jnp.concatenate([top[1:], jnp.zeros_like(top[:1])], axis=0)
        factors = interface[pole_index]
        below = jax.vmap(complex_product)(factors[:, 0], bottom) - jax.vmap(complex_product)(factors[:, 1], top_next)
        above = top_next - jax.vmap(complex_product)(factors[:, 2], below)
        above = above.at[PARTS_SIZE - 1].set(0.0)
        lifted = jax.vmap(transposed_product)(links, below)
        arriving = jnp.concatenate([jnp.zeros_like(lifted[:1]), lifted[:-1]], axis=0)
        update = source.at[:, 0].add(arriving)
        update = update.at[:, PB - 1].add(jax.vmap(real_product)(links, above))
        second = jax.vmap(partition_solve)(inverse, coupling, update)
        real_z = pole_values[pole_index, 0]
        imag_z = pole_values[pole_index, 1]
        real_w = pole_values[pole_index, 2]
        imag_w = pole_values[pole_index, 3]
        real_x = second[..., :M]
        imag_x = second[..., M:]
        basis_sum = basis_sum + (real_w * real_x - imag_w * imag_x)
        shifted_sum = shifted_sum + ((real_w * real_z - imag_w * imag_z) * real_x - (real_w * imag_z + imag_w * real_z) * imag_x - real_w * real_start)
    flat = basis_sum.reshape(ROWS, M)
    shifted = shifted_sum.reshape(ROWS, M)
    gram = inner_products(flat, flat) / ROWS
    projected = inner_products(flat, shifted) / ROWS
    factor = jnp.linalg.cholesky(gram)
    filtered_basis = lower_solve(factor, flat.T).T.reshape(PARTS_SIZE, PB, B, M)
    middle = lower_solve(factor, projected)
    rayleigh = lower_solve(factor, middle.T).T
    return (filtered_basis, rayleigh)
```

```python
import functools
import jax
import jax.numpy as jnp
from jax import lax
from jax.experimental import pallas as pl
from jax.experimental.pallas import tpu as pltpu
from jax.sharding import PartitionSpec as P

F32 = jnp.float32
BF16 = jnp.bfloat16
LANES = 128


def shifted(x, axis, by):
    length = lax.axis_size(axis)
    pairs = [(i, i + by) for i in range(length) if 0 <= i + by < length]
    return lax.ppermute(x, axis, pairs)


def flipped(x, axis, mask):
    return lax.ppermute(x, axis, [(i, i ^ mask) for i in range(lax.axis_size(axis))])


def complex_apply(stacked, vectors):
    order = stacked.shape[0] // 2
    width = vectors.shape[1] // 2
    out = jnp.dot(stacked, vectors.astype(BF16), preferred_element_type=F32)
    real = out[:order, :width] - out[order:, width:]
    imag = out[:order, width:] + out[order:, :width]
    return jnp.concatenate([real, imag], axis=1)


def real_apply(matrix, vectors):
    return jnp.dot(matrix, vectors.astype(BF16), preferred_element_type=F32)


def transposed_apply(matrix, vectors):
    return lax.dot_general(
        matrix, vectors.astype(BF16), (((0,), (0,)), ((), ())), preferred_element_type=F32
    )


def block_copies(k, lane, f_hbm, g_hbm, u_hbm, fv, gv, uv, sem):
    width = fv.shape[2]
    return (
        pltpu.make_async_copy(f_hbm.at[k, :, pl.ds(lane, width)], fv.at[k], sem.at[0, k]),
        pltpu.make_async_copy(g_hbm.at[k], gv.at[k], sem.at[1, k]),
        pltpu.make_async_copy(u_hbm.at[k], uv.at[k], sem.at[2, k]),
    )


def first_kernel(lane, f_hbm, g_hbm, u_hbm, s_ref, top_ref, sb_ref, fv, gv, uv, ut, hold, sem):
    blocks = gv.shape[0]
    copies = functools.partial(
        block_copies, lane=lane, f_hbm=f_hbm, g_hbm=g_hbm, u_hbm=u_hbm, fv=fv, gv=gv, uv=uv, sem=sem
    )
    for k in range(blocks):
        for copy in copies(k):
            copy.start()
    order = uv.shape[1]
    for copy in copies(0):
        copy.wait()
    out = jnp.dot(gv[0], fv[0], preferred_element_type=F32)
    hold[0] = jnp.concatenate([out[:order], out[order:]], axis=1)
    ut[0] = uv[0].T

    def forward(k, carry):
        for copy in copies(k):
            copy.wait()
        coupled = real_apply(ut[(k + 1) % 2], hold[k - 1])
        given = fv[k].astype(F32)
        hold[k] = complex_apply(
            gv[k], coupled + jnp.concatenate([given, jnp.zeros_like(given)], axis=1)
        )
        ut[k % 2] = uv[k].T
        return carry

    lax.fori_loop(1, blocks, forward, 0)
    sb_ref[...] = complex_apply(s_ref[...], hold[blocks - 1])

    def backward(i, carry):
        k = blocks - 2 - i
        hold[k] = hold[k] + complex_apply(gv[k], real_apply(uv[k], hold[k + 1]))
        return carry

    lax.fori_loop(0, blocks - 1, backward, 0)
    top_ref[...] = hold[0]


def first_solve(chunk, width, source, inverse, coupled, s_factor):
    blocks, stacked, order = inverse.shape
    tip = jax.ShapeDtypeStruct((order, 2 * width), F32)
    hbm = pl.BlockSpec(memory_space=pl.ANY)
    vmem = pl.BlockSpec(memory_space=pltpu.VMEM)
    flops = 2 * order * order * 2 * width * (5 * blocks - 3)
    return pl.pallas_call(
        functools.partial(first_kernel, chunk * width),
        out_shape=(tip, tip),
        in_specs=[hbm, hbm, hbm, vmem],
        out_specs=(vmem, vmem),
        scratch_shapes=[
            pltpu.VMEM((blocks, order, width), BF16),
            pltpu.VMEM((blocks, stacked, order), BF16),
            pltpu.VMEM((blocks, order, order), BF16),
            pltpu.VMEM((2, order, order), BF16),
            pltpu.VMEM((blocks, order, 2 * width), F32),
            pltpu.SemaphoreType.DMA((3, blocks)),
        ],
        cost_estimate=pl.CostEstimate(flops=flops, transcendentals=0, bytes_accessed=12 * 2**20),
        name="first_solve",
    )(source, inverse, coupled, s_factor)


def interface_kernel(last_ref, sb_ref, next_ref, k_ref, w_ref, link_ref, lifted_ref, added_ref):
    top_next = next_ref[...]
    below = sb_ref[...] - complex_apply(k_ref[...], top_next)
    lifted_ref[...] = transposed_apply(link_ref[...], below)
    above = top_next - complex_apply(w_ref[...], below)
    above = jnp.where(last_ref[0] == 1, jnp.zeros_like(above), above)
    added_ref[...] = real_apply(link_ref[...], above)


def interface_step(topmost, s_times, top_next, k_factor, w_factor, link):
    shape = jax.ShapeDtypeStruct(top_next.shape, F32)
    order, width = top_next.shape
    vmem = pl.BlockSpec(memory_space=pltpu.VMEM)
    return pl.pallas_call(
        interface_kernel,
        out_shape=(shape, shape),
        in_specs=[pl.BlockSpec(memory_space=pltpu.SMEM)] + [vmem] * 5,
        out_specs=(vmem, vmem),
        cost_estimate=pl.CostEstimate(
            flops=12 * order * order * width, transcendentals=0, bytes_accessed=4 * 2**20
        ),
        name="interface_step",
    )(topmost, s_times, top_next, k_factor, w_factor, link)


def second_kernel(
    lane, owners, place_ref, scale_ref, f_hbm, g_hbm, u_hbm, arrive_ref, added_ref,
    keep_y, keep_z, send_y, send_z, fv, gv, uv, ut, hold, sem,
):
    blocks = gv.shape[0]
    count = blocks // owners
    copies = functools.partial(
        block_copies, lane=lane, f_hbm=f_hbm, g_hbm=g_hbm, u_hbm=u_hbm, fv=fv, gv=gv, uv=uv, sem=sem
    )
    for k in range(blocks):
        for copy in copies(k):
            copy.start()
    width = fv.shape[2]

    def given(k):
        real = fv[k].astype(F32)
        return jnp.concatenate([real, jnp.zeros_like(real)], axis=1)

    for copy in copies(0):
        copy.wait()
    hold[0] = complex_apply(gv[0], given(0) + arrive_ref[...])
    ut[0] = uv[0].T

    def forward(k, carry):
        for copy in copies(k):
            copy.wait()
        coupled = real_apply(ut[(k + 1) % 2], hold[k - 1])
        hold[k] = complex_apply(gv[k], given(k) + coupled)
        ut[k % 2] = uv[k].T
        return carry

    lax.fori_loop(1, blocks - 1, forward, 0)
    last = blocks - 1
    for copy in copies(last):
        copy.wait()
    coupled = real_apply(ut[(last + 1) % 2], hold[last - 1])
    hold[last] = complex_apply(gv[last], (given(last) + added_ref[...]) + coupled)

    wr, wi, zwr, zwi = scale_ref[0], scale_ref[1], scale_ref[2], scale_ref[3]
    low = place_ref[0]
    high = place_ref[1]

    def emit(k, x):
        real, imag = x[:, :width], x[:, width:]
        y = wr * real - wi * imag
        z = zwr * real - zwi * imag - wr * fv[k].astype(F32)
        owner = k // count
        slot = ((owner // 2) ^ high) * count + k % count

        @pl.when(owner % 2 == low)
        def _():
            keep_y[slot] = y
            keep_z[slot] = z

        @pl.when(owner % 2 != low)
        def _():
            send_y[slot] = y
            send_z[slot] = z

    emit(last, hold[last])

    def backward(i, carry):
        k = blocks - 2 - i
        x = hold[k] + complex_apply(gv[k], real_apply(uv[k], hold[k + 1]))
        hold[k] = x
        emit(k, x)
        return carry

    lax.fori_loop(0, blocks - 1, backward, 0)


def second_solve(chunk, width, owners, place, scales, source, inverse, coupled, arriving, added):
    blocks, stacked, order = inverse.shape
    part = jax.ShapeDtypeStruct((blocks // 2, order, width), F32)
    hbm = pl.BlockSpec(memory_space=pl.ANY)
    vmem = pl.BlockSpec(memory_space=pltpu.VMEM)
    smem = pl.BlockSpec(memory_space=pltpu.SMEM)
    flops = 2 * order * order * 2 * width * (5 * blocks - 3)
    return pl.pallas_call(
        functools.partial(second_kernel, chunk * width, owners),
        out_shape=(part,) * 4,
        in_specs=[smem, smem, hbm, hbm, hbm, vmem, vmem],
        out_specs=(vmem,) * 4,
        scratch_shapes=[
            pltpu.VMEM((blocks, order, width), BF16),
            pltpu.VMEM((blocks, stacked, order), BF16),
            pltpu.VMEM((blocks, order, order), BF16),
            pltpu.VMEM((2, order, order), BF16),
            pltpu.VMEM((blocks, order, 2 * width), F32),
            pltpu.SemaphoreType.DMA((3, blocks)),
        ],
        cost_estimate=pl.CostEstimate(flops=flops, transcendentals=0, bytes_accessed=16 * 2**20),
        name="second_solve",
    )(place, scales, source, inverse, coupled, arriving, added)


def lower_solve(factor, right_side):
    return lax.linalg.triangular_solve(factor, right_side, left_side=True, lower=True)


def inner_products(left, right_side):
    return lax.dot_general(
        left,
        right_side,
        (((0,), (0,)), ((), ())),
        precision=lax.Precision.HIGHEST,
        preferred_element_type=F32,
    )


def summed_everywhere(x, steps, far):
    kept = []
    for axis, mask in steps:
        half = x.shape[0] // 2
        bit = (lax.axis_index(axis) // mask) % 2
        mine = lax.dynamic_slice_in_dim(x, bit * half, half, 0)
        other = lax.dynamic_slice_in_dim(x, (1 - bit) * half, half, 0)
        x = mine + flipped(other, axis, mask)
        kept.append(bit)
    axis, masks = far
    x = x + sum(flipped(x, axis, mask) for mask in masks)
    for (axis, mask), bit in zip(reversed(steps), reversed(kept)):
        other = flipped(x, axis, mask)
        x = jnp.where(bit == 0, jnp.concatenate([x, other]), jnp.concatenate([other, x]))
    return x


def on_device(initial_block, coupling, pivots, interface, pole_values):
    blocks = coupling.shape[1]
    order = coupling.shape[2]
    vectors = initial_block.shape[3]
    width = min(LANES, vectors)
    owners = lax.axis_size("pole")
    parts = lax.axis_size("dom")
    count = blocks // owners
    source = initial_block[0]
    coupled = coupling[0]
    inverse = pivots[0, 0].reshape(blocks, 2 * order, order)
    factors = interface[0, 0].reshape(3, 2 * order, order)
    link = coupled[blocks - 1]
    pole = lax.axis_index("pole")
    dom = lax.axis_index("dom")
    topmost = (dom == parts - 1).astype(jnp.int32).reshape(1)
    place = jnp.stack([pole % 2, pole // 2]).astype(jnp.int32)
    real_z, imag_z, real_w, imag_w = (pole_values[0, i] for i in range(4))
    scales = jnp.stack(
        [real_w, imag_w, real_w * real_z - imag_w * imag_z, real_w * imag_z + imag_w * real_z]
    )
    chunks = vectors // width
    firsts = [first_solve(c, width, source, inverse, coupled, factors[0]) for c in range(chunks)]
    tops = [shifted(top, "dom", -1) for top, _ in firsts]
    middles = [
        interface_step(topmost, firsts[c][1], tops[c], factors[1], factors[2], link)
        for c in range(chunks)
    ]
    arrivals = [shifted(lifted, "dom", 1) for lifted, _ in middles]
    seconds = [
        second_solve(c, width, owners, place, scales, source, inverse, coupled, arrivals[c], middles[c][1])
        for c in range(chunks)
    ]

    def gathered(keep, send):
        part = keep + flipped(send, "pole", 1)
        mask = 2
        while mask < owners:
            half = part.shape[0] // 2
            part = part[:half] + flipped(part[half:], "pole", mask)
            mask *= 2
        return part.reshape(count * order, width)

    own_y = jnp.concatenate([gathered(s[0], s[2]) for s in seconds], axis=1)
    own_z = jnp.concatenate([gathered(s[1], s[3]) for s in seconds], axis=1)
    gram_part = inner_products(own_y, own_y)
    projected_part = inner_products(own_y, own_z)
    both = jnp.concatenate([gram_part, projected_part], axis=1)
    near = [("pole", 1 << i) for i in range(owners.bit_length() - 1)] + [("dom", 1)]
    both = summed_everywhere(both, near, ("dom", tuple(range(2, parts, 2))))
    row_total = blocks * order * parts
    gram = both[:, :vectors] / row_total
    projected = both[:, vectors:] / row_total
    factor = jnp.linalg.cholesky(gram)
    filtered_basis = lower_solve(factor, own_y.T).T.reshape(1, count, order, vectors)
    middle = lower_solve(factor, projected)
    rayleigh = lower_solve(factor, middle.T).T
    return (filtered_basis, rayleigh)


def solution(mesh):
    in_specs = (
        P("dom", None, None, None),
        P("dom", None, None, None),
        P("pole", "dom", None, None, None, None),
        P("pole", "dom", None, None, None, None),
        P("pole", None),
    )
    out_specs = (P("dom", "pole", None, None), P())
    return jax.shard_map(
        on_device, mesh=mesh, in_specs=in_specs, out_specs=out_specs, check_vma=False
    )
```

```python
import functools
import jax
import jax.numpy as jnp
from jax import lax
from jax.experimental import pallas as pl
from jax.experimental.pallas import tpu as pltpu
from jax.sharding import PartitionSpec as P


F32 = jnp.float32
BF16 = jnp.bfloat16
LANES = 128
AHEAD = 3
STEP = 16
HIGHEST = lax.Precision.HIGHEST


def shifted(x, axis, by):
    length = lax.axis_size(axis)
    pairs = [(i, i + by) for i in range(length) if 0 <= i + by < length]
    return lax.ppermute(x, axis, pairs)


def flipped(x, axis, mask):
    return lax.ppermute(x, axis, [(i, i ^ mask) for i in range(lax.axis_size(axis))])


def complex_apply(stacked, vectors):
    order = stacked.shape[0] // 2
    width = vectors.shape[1] // 2
    out = jnp.dot(stacked, vectors.astype(BF16), preferred_element_type=F32)
    real = out[:order, :width] - out[order:, width:]
    imag = out[:order, width:] + out[order:, :width]
    return jnp.concatenate([real, imag], axis=1)


def real_apply(matrix, vectors):
    return jnp.dot(matrix, vectors.astype(BF16), preferred_element_type=F32)


def transposed_apply(matrix, vectors):
    return lax.dot_general(
        matrix, vectors.astype(BF16), (((0,), (0,)), ((), ())), preferred_element_type=F32
    )


def block_copies(k, f_hbm, g_hbm, u_hbm, fv, gv, uv, sem):
    return (
        pltpu.make_async_copy(f_hbm.at[k], fv.at[k], sem.at[0, k]),
        pltpu.make_async_copy(g_hbm.at[k], gv.at[k], sem.at[1, k]),
        pltpu.make_async_copy(u_hbm.at[k], uv.at[k], sem.at[2, k]),
    )


def fetch_ahead(blocks, copies, k):
    @pl.when(k + AHEAD < blocks)
    def _():
        for copy in copies(k + AHEAD):
            copy.start()


def first_kernel(groups, f_hbm, g_hbm, u_hbm, i_hbm, *refs):
    tops, sbs = refs[:groups], refs[groups : 2 * groups]
    fv, gv, uv, sv, ut, hold, sem, s_sem = refs[2 * groups :]
    blocks = gv.shape[0]
    order = uv.shape[1]
    width = fv.shape[2] // groups
    lanes = [slice(c * width, (c + 1) * width) for c in range(groups)]
    copies = functools.partial(
        block_copies, f_hbm=f_hbm, g_hbm=g_hbm, u_hbm=u_hbm, fv=fv, gv=gv, uv=uv, sem=sem
    )
    fetch = functools.partial(fetch_ahead, blocks, copies)
    for k in range(min(AHEAD, blocks)):
        for copy in copies(k):
            copy.start()
    s_copy = pltpu.make_async_copy(i_hbm.at[0], sv, s_sem)
    for copy in copies(0):
        copy.wait()
    for c in range(groups):
        out = jnp.dot(gv[0], fv[0, :, lanes[c]], preferred_element_type=F32)
        hold[c, 0] = jnp.concatenate([out[:order], out[order:]], axis=1)
    ut[0] = uv[0].T

    fetch(0)

    def forward(k, carry):
        fetch(k)
        for copy in copies(k):
            copy.wait()
        coupled = [real_apply(ut[(k + 1) % 2], hold[c, k - 1]) for c in range(groups)]
        for c in range(groups):
            given = fv[k, :, lanes[c]].astype(F32)
            hold[c, k] = complex_apply(
                gv[k], coupled[c] + jnp.concatenate([given, jnp.zeros_like(given)], axis=1)
            )
        ut[k % 2] = uv[k].T
        return carry

    s_copy.start()
    lax.fori_loop(1, blocks, forward, 0)
    s_copy.wait()
    for c in range(groups):
        sbs[c][...] = complex_apply(sv[...], hold[c, blocks - 1])

    def backward(i, carry):
        k = blocks - 2 - i
        coupled = [real_apply(uv[k], hold[c, k + 1]) for c in range(groups)]
        for c in range(groups):
            hold[c, k] = hold[c, k] + complex_apply(gv[k], coupled[c])
        return carry

    lax.fori_loop(0, blocks - 1, backward, 0)
    for c in range(groups):
        tops[c][...] = hold[c, 0]


def first_solve(groups, source, inverse, coupled, factors):
    blocks, stacked, order = inverse.shape
    vectors = source.shape[2]
    width = vectors // groups
    tip = jax.ShapeDtypeStruct((order, 2 * width), F32)
    hbm = pl.BlockSpec(memory_space=pl.ANY)
    vmem = pl.BlockSpec(memory_space=pltpu.VMEM)
    flops = 2 * order * order * 2 * vectors * (5 * blocks - 3)
    outs = pl.pallas_call(
        functools.partial(first_kernel, groups),
        out_shape=(tip,) * (2 * groups),
        in_specs=[hbm] * 4,
        out_specs=(vmem,) * (2 * groups),
        scratch_shapes=[
            pltpu.VMEM((blocks, order, vectors), BF16),
            pltpu.VMEM((blocks, stacked, order), BF16),
            pltpu.VMEM((blocks, order, order), BF16),
            pltpu.VMEM((stacked, order), BF16),
            pltpu.VMEM((2, order, order), BF16),
            pltpu.VMEM((groups, blocks, order, 2 * width), F32),
            pltpu.SemaphoreType.DMA((3, blocks)),
            pltpu.SemaphoreType.DMA,
        ],
        cost_estimate=pl.CostEstimate(flops=flops, transcendentals=0, bytes_accessed=14 * 2**20),
        name="first_solve",
    )(source, inverse, coupled, factors)
    return outs[:groups], outs[groups:]


def below_kernel(sb_hbm, next_hbm, i_hbm, u_hbm, below_ref, lifted_ref, sb, top_next, kv, uv, sem):
    copies = (
        pltpu.make_async_copy(next_hbm, top_next, sem.at[0]),
        pltpu.make_async_copy(i_hbm.at[1], kv, sem.at[1]),
        pltpu.make_async_copy(sb_hbm, sb, sem.at[2]),
        pltpu.make_async_copy(u_hbm.at[u_hbm.shape[0] - 1], uv, sem.at[3]),
    )
    for copy in copies:
        copy.start()
    copies[0].wait()
    copies[1].wait()
    product = complex_apply(kv[...], top_next[...])
    copies[2].wait()
    below = sb[...] - product
    below_ref[...] = below
    copies[3].wait()
    lifted_ref[...] = transposed_apply(uv[...], below)


def interface_below(s_times, top_next, factors, coupled):
    shape = jax.ShapeDtypeStruct(top_next.shape, F32)
    order, width = top_next.shape
    vmem = pl.BlockSpec(memory_space=pltpu.VMEM)
    hbm = pl.BlockSpec(memory_space=pl.ANY)
    return pl.pallas_call(
        below_kernel,
        out_shape=(shape, shape),
        in_specs=[hbm] * 4,
        out_specs=(vmem, vmem),
        scratch_shapes=[
            pltpu.VMEM(top_next.shape, F32),
            pltpu.VMEM(top_next.shape, F32),
            pltpu.VMEM((2 * order, order), BF16),
            pltpu.VMEM((order, order), BF16),
            pltpu.SemaphoreType.DMA((4,)),
        ],
        cost_estimate=pl.CostEstimate(
            flops=6 * order * order * width, transcendentals=0, bytes_accessed=4 * 2**20
        ),
        name="interface_below",
    )(s_times, top_next, factors, coupled)


def above_kernel(last_ref, below_ref, next_ref, i_hbm, u_hbm, added_ref, wv, uv, sem):
    copies = (
        pltpu.make_async_copy(i_hbm.at[2], wv, sem.at[0]),
        pltpu.make_async_copy(u_hbm.at[u_hbm.shape[0] - 1], uv, sem.at[1]),
    )
    for copy in copies:
        copy.start()
    copies[0].wait()
    above = next_ref[...] - complex_apply(wv[...], below_ref[...])
    above = jnp.where(last_ref[0] == 1, jnp.zeros_like(above), above)
    copies[1].wait()
    added_ref[...] = real_apply(uv[...], above)


def interface_above(topmost, below, top_next, factors, coupled):
    order, width = top_next.shape
    vmem = pl.BlockSpec(memory_space=pltpu.VMEM)
    hbm = pl.BlockSpec(memory_space=pl.ANY)
    return pl.pallas_call(
        above_kernel,
        out_shape=jax.ShapeDtypeStruct(top_next.shape, F32),
        in_specs=[pl.BlockSpec(memory_space=pltpu.SMEM), vmem, vmem, hbm, hbm],
        out_specs=vmem,
        scratch_shapes=[
            pltpu.VMEM((2 * order, order), BF16),
            pltpu.VMEM((order, order), BF16),
            pltpu.SemaphoreType.DMA((2,)),
        ],
        cost_estimate=pl.CostEstimate(
            flops=6 * order * order * width, transcendentals=0, bytes_accessed=4 * 2**20
        ),
        name="interface_above",
    )(topmost, below, top_next, factors, coupled)


def second_kernel(
    lane, owners, place_ref, scale_ref, f_hbm, g_hbm, u_hbm, arrive_hbm, added_hbm,
    keep_y, keep_z, send_y, send_z, fv, gv, uv, ut, hold, yv, zv, arrive, added, sem, out_sem, tip_sem,
):
    blocks = gv.shape[0]
    count = blocks // owners
    width = fv.shape[2]
    copies = functools.partial(
        block_copies, f_hbm=f_hbm.at[:, :, pl.ds(lane, width)], g_hbm=g_hbm, u_hbm=u_hbm,
        fv=fv, gv=gv, uv=uv, sem=sem,
    )
    fetch = functools.partial(fetch_ahead, blocks, copies)
    for k in range(min(AHEAD, blocks)):
        for copy in copies(k):
            copy.start()

    arrive_copy = pltpu.make_async_copy(arrive_hbm, arrive, tip_sem.at[0])
    added_copy = pltpu.make_async_copy(added_hbm, added, tip_sem.at[1])
    arrive_copy.start()

    def given(k):
        real = fv[k].astype(F32)
        return jnp.concatenate([real, jnp.zeros_like(real)], axis=1)

    for copy in copies(0):
        copy.wait()
    arrive_copy.wait()
    hold[0] = complex_apply(gv[0], given(0) + arrive[...])
    added_copy.start()
    ut[0] = uv[0].T

    fetch(0)

    def forward(k, carry):
        fetch(k)
        for copy in copies(k):
            copy.wait()
        coupled = real_apply(ut[(k + 1) % 2], hold[k - 1])
        hold[k] = complex_apply(gv[k], given(k) + coupled)
        ut[k % 2] = uv[k].T
        return carry

    lax.fori_loop(1, blocks - 1, forward, 0)
    last = blocks - 1
    for copy in copies(last):
        copy.wait()
    added_copy.wait()
    coupled = real_apply(ut[(last + 1) % 2], hold[last - 1])
    hold[last] = complex_apply(gv[last], (given(last) + added[...]) + coupled)

    wr, wi, zwr, zwi = scale_ref[0], scale_ref[1], scale_ref[2], scale_ref[3]
    low = place_ref[0]
    high = place_ref[1]

    def emit(k, x):
        real, imag = x[:, :width], x[:, width:]
        y = wr * real - wi * imag
        z = zwr * real - zwi * imag - wr * fv[k].astype(F32)
        owner = k // count
        slot = ((owner // 2) ^ high) * count + k % count

        yv[k] = y
        zv[k] = z

        @pl.when(owner % 2 == low)
        def _():
            pltpu.make_async_copy(yv.at[k], keep_y.at[slot], out_sem.at[0, k]).start()
            pltpu.make_async_copy(zv.at[k], keep_z.at[slot], out_sem.at[1, k]).start()

        @pl.when(owner % 2 != low)
        def _():
            pltpu.make_async_copy(yv.at[k], send_y.at[slot], out_sem.at[0, k]).start()
            pltpu.make_async_copy(zv.at[k], send_z.at[slot], out_sem.at[1, k]).start()

    emit(last, hold[last])

    def backward(i, carry):
        k = blocks - 2 - i
        x = hold[k] + complex_apply(gv[k], real_apply(uv[k], hold[k + 1]))
        hold[k] = x
        emit(k, x)
        return carry

    lax.fori_loop(0, blocks - 1, backward, 0)
    for k in range(blocks):
        pltpu.make_async_copy(yv.at[k], keep_y.at[0], out_sem.at[0, k]).wait()
        pltpu.make_async_copy(zv.at[k], keep_z.at[0], out_sem.at[1, k]).wait()


def second_solve(chunk, width, owners, place, scales, source, inverse, coupled, arriving, added):
    blocks, stacked, order = inverse.shape
    part = jax.ShapeDtypeStruct((blocks // 2, order, width), F32)
    hbm = pl.BlockSpec(memory_space=pl.ANY)
    vmem = pl.BlockSpec(memory_space=pltpu.VMEM)
    smem = pl.BlockSpec(memory_space=pltpu.SMEM)
    flops = 2 * order * order * 2 * width * (5 * blocks - 3)
    return pl.pallas_call(
        functools.partial(second_kernel, chunk * width, owners),
        out_shape=(part,) * 4,
        in_specs=[smem, smem] + [hbm] * 5,
        out_specs=(hbm,) * 4,
        scratch_shapes=[
            pltpu.VMEM((blocks, order, width), BF16),
            pltpu.VMEM((blocks, stacked, order), BF16),
            pltpu.VMEM((blocks, order, order), BF16),
            pltpu.VMEM((2, order, order), BF16),
            pltpu.VMEM((blocks, order, 2 * width), F32),
            pltpu.VMEM((blocks, order, width), F32),
            pltpu.VMEM((blocks, order, width), F32),
            pltpu.VMEM((order, 2 * width), F32),
            pltpu.VMEM((order, 2 * width), F32),
            pltpu.SemaphoreType.DMA((3, blocks)),
            pltpu.SemaphoreType.DMA((2, blocks)),
            pltpu.SemaphoreType.DMA((2,)),
        ],
        cost_estimate=pl.CostEstimate(flops=flops, transcendentals=0, bytes_accessed=16 * 2**20),
        name="second_solve",
    )(place, scales, source, inverse, coupled, arriving, added)


def factor_kernel(total, gram_ref, y_ref, basis_ref, inverse_ref, acc):
    n = gram_ref.shape[0]
    rows = lax.broadcasted_iota(jnp.int32, (n, n), 0)
    cols = lax.broadcasted_iota(jnp.int32, (n, n), 1)
    acc[:, :n] = gram_ref[...] / total
    acc[:, n:] = (rows == cols).astype(F32)
    lane = 128
    row = lax.broadcasted_iota(jnp.int32, (STEP, lane), 0)
    for r in range(0, n, STEP):
        low = r // lane * lane
        high = (r + STEP + lane - 1) // lane * lane
        panel = acc[r : r + STEP, low : n + high]
        tiles = [panel[:, i:i+lane] for i in range(0, panel.shape[1], lane)]
        cols_ = [jnp.broadcast_to(panel[:, r-low+j:r-low+j+1], (STEP, lane)) for j in range(STEP)]
        scale = jnp.ones((STEP, lane), F32)
        for k in range(STEP):
            inv = lax.rsqrt(jnp.broadcast_to(cols_[k][k:k+1], (STEP, lane)))
            scale = jnp.where(row == k, inv, scale)
            m = jnp.where(row > k, cols_[k], 0.0) * (inv * inv)
            for j in range(k + 1, STEP):
                cols_[j] = cols_[j] - m * jnp.broadcast_to(cols_[j][k:k+1], (STEP, lane))
            tiles = [t - m * jnp.broadcast_to(t[k:k+1], (STEP, lane)) for t in tiles]
        done = jnp.concatenate([t * scale for t in tiles], axis=1)
        acc[r : r + STEP, low : n + high] = done
        if r + STEP < n:
            left = done[:, :n-low].T[r+STEP-low:]
            acc[r+STEP:, low : n + high] -= jnp.dot(left, done, precision=HIGHEST, preferred_element_type=F32)
    inverse = jnp.where(cols <= rows, acc[:, n:], 0.0)
    nt = (((1,), (1,)), ((), ()))
    basis_ref[...] = lax.dot_general(y_ref[...], inverse, nt, precision=HIGHEST, preferred_element_type=F32)
    inverse_ref[...] = inverse


def congruence_kernel(total, inverse_ref, proj_ref, ray_ref):
    inverse = inverse_ref[...]
    middle = jnp.dot(
        inverse, proj_ref[...] / total, precision=HIGHEST, preferred_element_type=F32
    )
    ray_ref[...] = lax.dot_general(
        middle, inverse, (((1,), (1,)), ((), ())), precision=HIGHEST, preferred_element_type=F32
    )


def congruence(total, inverse, projected):
    vmem = pl.BlockSpec(memory_space=pltpu.VMEM)
    return pl.pallas_call(
        functools.partial(congruence_kernel, float(total)),
        out_shape=jax.ShapeDtypeStruct(inverse.shape, F32),
        in_specs=[vmem] * 2,
        out_specs=vmem,
        cost_estimate=pl.CostEstimate(flops=2**30, transcendentals=0, bytes_accessed=2**20),
        name="congruence",
    )(inverse, projected)


def orthonormalized(total, gram, y):
    n = gram.shape[0]
    vmem = pl.BlockSpec(memory_space=pltpu.VMEM)
    return pl.pallas_call(
        functools.partial(factor_kernel, float(total)),
        out_shape=(jax.ShapeDtypeStruct(y.shape, F32), jax.ShapeDtypeStruct((n, n), F32)),
        in_specs=[vmem] * 2,
        out_specs=(vmem, vmem),
        scratch_shapes=[pltpu.VMEM((n, 2 * n), F32)],
        cost_estimate=pl.CostEstimate(
            flops=12 * 2**30, transcendentals=0, bytes_accessed=3 * 2**20
        ),
        name="orthonormalized",
    )(gram, y)


def inner_products(left, right_side):
    return lax.dot_general(
        left,
        right_side,
        (((0,), (0,)), ((), ())),
        precision=lax.Precision.HIGHEST,
        preferred_element_type=F32,
    )


def summed_everywhere(x, steps, far):
    kept = []
    for axis, mask in steps:
        half = x.shape[0] // 2
        bit = (lax.axis_index(axis) // mask) % 2
        mine = lax.dynamic_slice_in_dim(x, bit * half, half, 0)
        other = lax.dynamic_slice_in_dim(x, (1 - bit) * half, half, 0)
        x = mine + flipped(other, axis, mask)
        kept.append(bit)
    axis, masks = far
    x = x + sum(flipped(x, axis, mask) for mask in masks)
    for (axis, mask), bit in zip(reversed(steps), reversed(kept)):
        other = flipped(x, axis, mask)
        x = jnp.where(bit == 0, jnp.concatenate([x, other]), jnp.concatenate([other, x]))
    return x


def on_device(initial_block, coupling, pivots, interface, pole_values):
    blocks = coupling.shape[1]
    order = coupling.shape[2]
    vectors = initial_block.shape[3]
    width = min(LANES, vectors)
    owners = lax.axis_size("pole")
    parts = lax.axis_size("dom")
    count = blocks // owners
    source = initial_block[0]
    coupled = coupling[0]
    inverse = pivots[0, 0].reshape(blocks, 2 * order, order)
    factors = interface[0, 0].reshape(3, 2 * order, order)
    pole = lax.axis_index("pole")
    dom = lax.axis_index("dom")
    topmost = (dom == parts - 1).astype(jnp.int32).reshape(1)
    place = jnp.stack([pole % 2, pole // 2]).astype(jnp.int32)
    real_z, imag_z, real_w, imag_w = (pole_values[0, i] for i in range(4))
    scales = jnp.stack(
        [real_w, imag_w, real_w * real_z - imag_w * imag_z, real_w * imag_z + imag_w * real_z]
    )
    chunks = vectors // width
    tips, s_times = first_solve(chunks, source, inverse, coupled, factors)
    tops, belows, arrivals, added = [], [], [], []
    for c in range(chunks):
        tops.append(shifted(tips[c], "dom", -1))
    for c in range(chunks):
        belows.append(interface_below(s_times[c], tops[c], factors, coupled))
        arrivals.append(shifted(belows[c][1], "dom", 1))
        added.append(interface_above(topmost, belows[c][0], tops[c], factors, coupled))
    masks = [1 << i for i in range(1, owners.bit_length() - 1)]

    def pole_sum(keep, send):
        other = flipped(send, "pole", 1)
        terms = [keep, other]
        for mask in masks:
            half = terms[0].shape[0] // 2
            out = sum(term[half:] for term in terms)
            terms = [term[:half] for term in terms] + [flipped(out, "pole", mask)]
        return sum(terms).reshape(count * order, width)

    own_y, own_z = [], []
    for c in range(chunks):
        keep_y, keep_z, send_y, send_z = second_solve(
            c, width, owners, place, scales, source, inverse, coupled, arrivals[c], added[c]
        )
        own_y.append(pole_sum(keep_y, send_y))
        own_z.append(pole_sum(keep_z, send_z))
    own_y = jnp.concatenate(own_y, axis=1)
    own_z = jnp.concatenate(own_z, axis=1)
    near = [("pole", 1 << i) for i in range(owners.bit_length() - 1)] + [("dom", 1)]
    far = ("dom", tuple(range(2, parts, 2)))
    gram = summed_everywhere(inner_products(own_y, own_y), near, far)
    projected = summed_everywhere(inner_products(own_y, own_z), near, far)
    row_total = blocks * order * parts
    basis, inverse_factor = orthonormalized(row_total, gram, own_y)
    rayleigh = congruence(row_total, inverse_factor, projected)
    return (basis.reshape(1, count, order, vectors), rayleigh)


def solution(mesh):
    in_specs = (
        P("dom", None, None, None),
        P("dom", None, None, None),
        P("pole", "dom", None, None, None, None),
        P("pole", "dom", None, None, None, None),
        P("pole", None),
    )
    out_specs = (P("dom", "pole", None, None), P())
    return jax.shard_map(
        on_device, mesh=mesh, in_specs=in_specs, out_specs=out_specs, check_vma=False
    )
```

```python
import functools
import jax
import jax.numpy as jnp
from jax import lax
from jax.experimental import pallas as pl
from jax.experimental.pallas import tpu as pltpu
from jax.sharding import PartitionSpec as P


F32 = jnp.float32
BF16 = jnp.bfloat16
LANES = 128
AHEAD = 3
STEP = 16
HIGHEST = lax.Precision.HIGHEST


def shifted(x, axis, by):
    length = lax.axis_size(axis)
    pairs = [(i, i + by) for i in range(length) if 0 <= i + by < length]
    return lax.ppermute(x, axis, pairs)


def flipped(x, axis, mask):
    return lax.ppermute(x, axis, [(i, i ^ mask) for i in range(lax.axis_size(axis))])


def complex_apply(stacked, vectors):
    order = stacked.shape[0] // 2
    width = vectors.shape[1] // 2
    out = jnp.dot(stacked, vectors.astype(BF16), preferred_element_type=F32)
    real = out[:order, :width] - out[order:, width:]
    imag = out[:order, width:] + out[order:, :width]
    return jnp.concatenate([real, imag], axis=1)


def real_apply(matrix, vectors):
    return jnp.dot(matrix, vectors.astype(BF16), preferred_element_type=F32)


def transposed_apply(matrix, vectors):
    return lax.dot_general(
        matrix, vectors.astype(BF16), (((0,), (0,)), ((), ())), preferred_element_type=F32
    )


def block_copies(k, f_hbm, g_hbm, u_hbm, fv, gv, uv, sem):
    return (
        pltpu.make_async_copy(f_hbm.at[k], fv.at[k], sem.at[0, k]),
        pltpu.make_async_copy(g_hbm.at[k], gv.at[k], sem.at[1, k]),
        pltpu.make_async_copy(u_hbm.at[k], uv.at[k], sem.at[2, k]),
    )


def fetch_ahead(blocks, copies, k):
    @pl.when(k + AHEAD < blocks)
    def _():
        for copy in copies(k + AHEAD):
            copy.start()


def first_kernel(groups, f_hbm, g_hbm, u_hbm, i_hbm, *refs):
    tops, sbs = refs[:groups], refs[groups : 2 * groups]
    fv, gv, uv, sv, ut, hold, sem, s_sem = refs[2 * groups :]
    blocks = gv.shape[0]
    order = uv.shape[1]
    width = fv.shape[2] // groups
    lanes = [slice(c * width, (c + 1) * width) for c in range(groups)]
    copies = functools.partial(
        block_copies, f_hbm=f_hbm, g_hbm=g_hbm, u_hbm=u_hbm, fv=fv, gv=gv, uv=uv, sem=sem
    )
    fetch = functools.partial(fetch_ahead, blocks, copies)
    for k in range(min(AHEAD, blocks)):
        for copy in copies(k):
            copy.start()
    s_copy = pltpu.make_async_copy(i_hbm.at[0], sv, s_sem)
    for copy in copies(0):
        copy.wait()
    for c in range(groups):
        out = jnp.dot(gv[0], fv[0, :, lanes[c]], preferred_element_type=F32)
        hold[c, 0] = jnp.concatenate([out[:order], out[order:]], axis=1)
    ut[0] = uv[0].T

    fetch(0)

    def forward(k, carry):
        fetch(k)
        for copy in copies(k):
            copy.wait()
        coupled = [real_apply(ut[(k + 1) % 2], hold[c, k - 1]) for c in range(groups)]
        for c in range(groups):
            given = fv[k, :, lanes[c]].astype(F32)
            hold[c, k] = complex_apply(
                gv[k], coupled[c] + jnp.concatenate([given, jnp.zeros_like(given)], axis=1)
            )
        ut[k % 2] = uv[k].T
        return carry

    s_copy.start()
    lax.fori_loop(1, blocks, forward, 0)
    s_copy.wait()
    for c in range(groups):
        sbs[c][...] = complex_apply(sv[...], hold[c, blocks - 1])

    def backward(i, carry):
        k = blocks - 2 - i
        coupled = [real_apply(uv[k], hold[c, k + 1]) for c in range(groups)]
        for c in range(groups):
            hold[c, k] = hold[c, k] + complex_apply(gv[k], coupled[c])
        return carry

    lax.fori_loop(0, blocks - 1, backward, 0)
    for c in range(groups):
        tops[c][...] = hold[c, 0]


def first_solve(groups, source, inverse, coupled, factors):
    blocks, stacked, order = inverse.shape
    vectors = source.shape[2]
    width = vectors // groups
    tip = jax.ShapeDtypeStruct((order, 2 * width), F32)
    hbm = pl.BlockSpec(memory_space=pl.ANY)
    vmem = pl.BlockSpec(memory_space=pltpu.VMEM)
    flops = 2 * order * order * 2 * vectors * (5 * blocks - 3)
    outs = pl.pallas_call(
        functools.partial(first_kernel, groups),
        out_shape=(tip,) * (2 * groups),
        in_specs=[hbm] * 4,
        out_specs=(vmem,) * (2 * groups),
        scratch_shapes=[
            pltpu.VMEM((blocks, order, vectors), BF16),
            pltpu.VMEM((blocks, stacked, order), BF16),
            pltpu.VMEM((blocks, order, order), BF16),
            pltpu.VMEM((stacked, order), BF16),
            pltpu.VMEM((2, order, order), BF16),
            pltpu.VMEM((groups, blocks, order, 2 * width), F32),
            pltpu.SemaphoreType.DMA((3, blocks)),
            pltpu.SemaphoreType.DMA,
        ],
        cost_estimate=pl.CostEstimate(flops=flops, transcendentals=0, bytes_accessed=14 * 2**20),
        name="first_solve",
    )(source, inverse, coupled, factors)
    return outs[:groups], outs[groups:]


def below_kernel(sb_hbm, next_hbm, i_hbm, u_hbm, below_ref, lifted_ref, sb, top_next, kv, uv, sem):
    copies = (
        pltpu.make_async_copy(next_hbm, top_next, sem.at[0]),
        pltpu.make_async_copy(i_hbm.at[1], kv, sem.at[1]),
        pltpu.make_async_copy(sb_hbm, sb, sem.at[2]),
        pltpu.make_async_copy(u_hbm.at[u_hbm.shape[0] - 1], uv, sem.at[3]),
    )
    for copy in copies:
        copy.start()
    copies[0].wait()
    copies[1].wait()
    product = complex_apply(kv[...], top_next[...])
    copies[2].wait()
    below = sb[...] - product
    below_ref[...] = below
    copies[3].wait()
    lifted_ref[...] = transposed_apply(uv[...], below)


def interface_below(s_times, top_next, factors, coupled):
    shape = jax.ShapeDtypeStruct(top_next.shape, F32)
    order, width = top_next.shape
    vmem = pl.BlockSpec(memory_space=pltpu.VMEM)
    hbm = pl.BlockSpec(memory_space=pl.ANY)
    return pl.pallas_call(
        below_kernel,
        out_shape=(shape, shape),
        in_specs=[hbm] * 4,
        out_specs=(vmem, vmem),
        scratch_shapes=[
            pltpu.VMEM(top_next.shape, F32),
            pltpu.VMEM(top_next.shape, F32),
            pltpu.VMEM((2 * order, order), BF16),
            pltpu.VMEM((order, order), BF16),
            pltpu.SemaphoreType.DMA((4,)),
        ],
        cost_estimate=pl.CostEstimate(
            flops=6 * order * order * width, transcendentals=0, bytes_accessed=4 * 2**20
        ),
        name="interface_below",
    )(s_times, top_next, factors, coupled)


def above_kernel(parts, below_hbm, next_hbm, i_hbm, u_hbm, added_ref, below, top_next, wv, uv, sem):
    copies = (
        pltpu.make_async_copy(below_hbm, below, sem.at[0]),
        pltpu.make_async_copy(i_hbm.at[2], wv, sem.at[1]),
        pltpu.make_async_copy(next_hbm, top_next, sem.at[2]),
        pltpu.make_async_copy(u_hbm.at[u_hbm.shape[0] - 1], uv, sem.at[3]),
    )
    for copy in copies:
        copy.start()
    for copy in copies[:3]:
        copy.wait()
    above = top_next[...] - complex_apply(wv[...], below[...])
    topmost = lax.axis_index("dom") == parts - 1
    above = jnp.where(topmost, jnp.zeros_like(above), above)
    copies[3].wait()
    added_ref[...] = real_apply(uv[...], above)


def interface_above(parts, below, top_next, factors, coupled):
    order, width = top_next.shape
    vmem = pl.BlockSpec(memory_space=pltpu.VMEM)
    hbm = pl.BlockSpec(memory_space=pl.ANY)
    return pl.pallas_call(
        functools.partial(above_kernel, parts),
        out_shape=jax.ShapeDtypeStruct(top_next.shape, F32),
        in_specs=[hbm] * 4,
        out_specs=vmem,
        scratch_shapes=[
            pltpu.VMEM(top_next.shape, F32),
            pltpu.VMEM(top_next.shape, F32),
            pltpu.VMEM((2 * order, order), BF16),
            pltpu.VMEM((order, order), BF16),
            pltpu.SemaphoreType.DMA((4,)),
        ],
        cost_estimate=pl.CostEstimate(
            flops=6 * order * order * width, transcendentals=0, bytes_accessed=4 * 2**20
        ),
        name="interface_above",
    )(below, top_next, factors, coupled)


def second_kernel(
    lane, owners, pole_ref, f_hbm, g_hbm, u_hbm, arrive_hbm, added_hbm,
    keep_y, keep_z, send_y, send_z, fv, gv, uv, ut, hold, yv, zv, arrive, added, sem, out_sem, tip_sem,
):
    blocks = gv.shape[0]
    count = blocks // owners
    width = fv.shape[2]
    copies = functools.partial(
        block_copies, f_hbm=f_hbm.at[:, :, pl.ds(lane, width)], g_hbm=g_hbm, u_hbm=u_hbm,
        fv=fv, gv=gv, uv=uv, sem=sem,
    )
    fetch = functools.partial(fetch_ahead, blocks, copies)
    for k in range(min(AHEAD, blocks)):
        for copy in copies(k):
            copy.start()

    arrive_copy = pltpu.make_async_copy(arrive_hbm, arrive, tip_sem.at[0])
    added_copy = pltpu.make_async_copy(added_hbm, added, tip_sem.at[1])
    arrive_copy.start()

    def given(k):
        real = fv[k].astype(F32)
        return jnp.concatenate([real, jnp.zeros_like(real)], axis=1)

    for copy in copies(0):
        copy.wait()
    arrive_copy.wait()
    hold[0] = complex_apply(gv[0], given(0) + arrive[...])
    added_copy.start()
    ut[0] = uv[0].T

    fetch(0)

    def forward(k, carry):
        fetch(k)
        for copy in copies(k):
            copy.wait()
        coupled = real_apply(ut[(k + 1) % 2], hold[k - 1])
        hold[k] = complex_apply(gv[k], given(k) + coupled)
        ut[k % 2] = uv[k].T
        return carry

    lax.fori_loop(1, blocks - 1, forward, 0)
    last = blocks - 1
    for copy in copies(last):
        copy.wait()
    added_copy.wait()
    coupled = real_apply(ut[(last + 1) % 2], hold[last - 1])
    hold[last] = complex_apply(gv[last], (given(last) + added[...]) + coupled)

    zr, zi, wr, wi = (pole_ref[0, i] for i in range(4))
    zwr = wr * zr - wi * zi
    zwi = wr * zi + wi * zr
    pole = lax.axis_index("pole")
    low = pole % 2
    high = pole // 2

    def emit(k, x):
        real, imag = x[:, :width], x[:, width:]
        y = wr * real - wi * imag
        z = zwr * real - zwi * imag - wr * fv[k].astype(F32)
        owner = k // count
        slot = ((owner // 2) ^ high) * count + k % count

        yv[k] = y
        zv[k] = z

        @pl.when(owner % 2 == low)
        def _():
            pltpu.make_async_copy(yv.at[k], keep_y.at[slot], out_sem.at[0, k]).start()
            pltpu.make_async_copy(zv.at[k], keep_z.at[slot], out_sem.at[1, k]).start()

        @pl.when(owner % 2 != low)
        def _():
            pltpu.make_async_copy(yv.at[k], send_y.at[slot], out_sem.at[0, k]).start()
            pltpu.make_async_copy(zv.at[k], send_z.at[slot], out_sem.at[1, k]).start()

    emit(last, hold[last])

    def backward(i, carry):
        k = blocks - 2 - i
        x = hold[k] + complex_apply(gv[k], real_apply(uv[k], hold[k + 1]))
        hold[k] = x
        emit(k, x)
        return carry

    lax.fori_loop(0, blocks - 1, backward, 0)
    for k in range(blocks):
        pltpu.make_async_copy(yv.at[k], keep_y.at[0], out_sem.at[0, k]).wait()
        pltpu.make_async_copy(zv.at[k], keep_z.at[0], out_sem.at[1, k]).wait()


def second_solve(chunk, width, owners, pole_values, source, inverse, coupled, arriving, added):
    blocks, stacked, order = inverse.shape
    part = jax.ShapeDtypeStruct((blocks // 2, order, width), F32)
    hbm = pl.BlockSpec(memory_space=pl.ANY)
    vmem = pl.BlockSpec(memory_space=pltpu.VMEM)
    smem = pl.BlockSpec(memory_space=pltpu.SMEM)
    flops = 2 * order * order * 2 * width * (5 * blocks - 3)
    return pl.pallas_call(
        functools.partial(second_kernel, chunk * width, owners),
        out_shape=(part,) * 4,
        in_specs=[smem] + [hbm] * 5,
        out_specs=(hbm,) * 4,
        scratch_shapes=[
            pltpu.VMEM((blocks, order, width), BF16),
            pltpu.VMEM((blocks, stacked, order), BF16),
            pltpu.VMEM((blocks, order, order), BF16),
            pltpu.VMEM((2, order, order), BF16),
            pltpu.VMEM((blocks, order, 2 * width), F32),
            pltpu.VMEM((blocks, order, width), F32),
            pltpu.VMEM((blocks, order, width), F32),
            pltpu.VMEM((order, 2 * width), F32),
            pltpu.VMEM((order, 2 * width), F32),
            pltpu.SemaphoreType.DMA((3, blocks)),
            pltpu.SemaphoreType.DMA((2, blocks)),
            pltpu.SemaphoreType.DMA((2,)),
        ],
        cost_estimate=pl.CostEstimate(flops=flops, transcendentals=0, bytes_accessed=16 * 2**20),
        name="second_solve",
    )(pole_values, source, inverse, coupled, arriving, added)


def factor_kernel(total, gram_ref, y_ref, basis_ref, inverse_ref, acc):
    n = gram_ref.shape[0]
    rows = lax.broadcasted_iota(jnp.int32, (n, n), 0)
    cols = lax.broadcasted_iota(jnp.int32, (n, n), 1)
    acc[:, :n] = gram_ref[...] / total
    acc[:, n:] = (rows == cols).astype(F32)
    lane = 128
    row = lax.broadcasted_iota(jnp.int32, (STEP, lane), 0)
    for r in range(0, n, STEP):
        low = r // lane * lane
        high = (r + STEP + lane - 1) // lane * lane
        panel = acc[r : r + STEP, low : n + high]
        tiles = [panel[:, i:i+lane] for i in range(0, panel.shape[1], lane)]
        cols_ = [jnp.broadcast_to(panel[:, r-low+j:r-low+j+1], (STEP, lane)) for j in range(STEP)]
        scale = jnp.ones((STEP, lane), F32)
        for k in range(STEP):
            inv = lax.rsqrt(jnp.broadcast_to(cols_[k][k:k+1], (STEP, lane)))
            scale = jnp.where(row == k, inv, scale)
            m = jnp.where(row > k, cols_[k], 0.0) * (inv * inv)
            for j in range(k + 1, STEP):
                cols_[j] = cols_[j] - m * jnp.broadcast_to(cols_[j][k:k+1], (STEP, lane))
            tiles = [t - m * jnp.broadcast_to(t[k:k+1], (STEP, lane)) for t in tiles]
        done = jnp.concatenate([t * scale for t in tiles], axis=1)
        acc[r : r + STEP, low : n + high] = done
        if r + STEP < n:
            left = done[:, :n-low].T[r+STEP-low:]
            acc[r+STEP:, low : n + high] -= jnp.dot(left, done, precision=HIGHEST, preferred_element_type=F32)
    inverse = jnp.where(cols <= rows, acc[:, n:], 0.0)
    nt = (((1,), (1,)), ((), ()))
    basis_ref[...] = lax.dot_general(y_ref[...], inverse, nt, precision=HIGHEST, preferred_element_type=F32)
    inverse_ref[...] = inverse


def congruence_kernel(total, inverse_ref, proj_ref, ray_ref):
    inverse = inverse_ref[...]
    middle = jnp.dot(
        inverse, proj_ref[...] / total, precision=HIGHEST, preferred_element_type=F32
    )
    ray_ref[...] = lax.dot_general(
        middle, inverse, (((1,), (1,)), ((), ())), precision=HIGHEST, preferred_element_type=F32
    )


def congruence(total, inverse, projected):
    vmem = pl.BlockSpec(memory_space=pltpu.VMEM)
    return pl.pallas_call(
        functools.partial(congruence_kernel, float(total)),
        out_shape=jax.ShapeDtypeStruct(inverse.shape, F32),
        in_specs=[vmem] * 2,
        out_specs=vmem,
        cost_estimate=pl.CostEstimate(flops=2**30, transcendentals=0, bytes_accessed=2**20),
        name="congruence",
    )(inverse, projected)


def orthonormalized(total, gram, y):
    n = gram.shape[0]
    vmem = pl.BlockSpec(memory_space=pltpu.VMEM)
    return pl.pallas_call(
        functools.partial(factor_kernel, float(total)),
        out_shape=(jax.ShapeDtypeStruct(y.shape, F32), jax.ShapeDtypeStruct((n, n), F32)),
        in_specs=[vmem] * 2,
        out_specs=(vmem, vmem),
        scratch_shapes=[pltpu.VMEM((n, 2 * n), F32)],
        cost_estimate=pl.CostEstimate(
            flops=12 * 2**30, transcendentals=0, bytes_accessed=3 * 2**20
        ),
        name="orthonormalized",
    )(gram, y)


def inner_products(left, right_side):
    return lax.dot_general(
        left,
        right_side,
        (((0,), (0,)), ((), ())),
        precision=lax.Precision.HIGHEST,
        preferred_element_type=F32,
    )


def summed_everywhere(x, near, far):
    kept = []
    for axis, i in near:
        half = x.shape[0] // 2
        upper = (lax.axis_index(axis) >> i) & 1 == 1
        mine = jnp.where(upper, x[half:], x[:half])
        other = jnp.where(upper, x[:half], x[half:])
        x = mine + flipped(other, axis, 1 << i)
        kept.append(upper)
    for axis, i in far:
        x = x + flipped(x, axis, 1 << i)
    for (axis, i), upper in zip(reversed(near), reversed(kept)):
        other = flipped(x, axis, 1 << i)
        x = jnp.where(upper, jnp.concatenate([other, x]), jnp.concatenate([x, other]))
    return x


def on_device(initial_block, coupling, pivots, interface, pole_values):
    blocks = coupling.shape[1]
    order = coupling.shape[2]
    vectors = initial_block.shape[3]
    width = min(LANES, vectors)
    owners = lax.axis_size("pole")
    parts = lax.axis_size("dom")
    count = blocks // owners
    source = initial_block[0]
    coupled = coupling[0]
    inverse = pivots[0, 0].reshape(blocks, 2 * order, order)
    factors = interface[0, 0].reshape(3, 2 * order, order)
    chunks = vectors // width
    tips, s_times = first_solve(chunks, source, inverse, coupled, factors)
    tops, belows, arrivals, added = [], [], [], []
    for c in range(chunks):
        tops.append(shifted(tips[c], "dom", -1))
    for c in range(chunks):
        belows.append(interface_below(s_times[c], tops[c], factors, coupled))
        arrivals.append(shifted(belows[c][1], "dom", 1))
        added.append(interface_above(parts, belows[c][0], tops[c], factors, coupled))
    masks = [1 << i for i in range(1, owners.bit_length() - 1)]

    def pole_sum(keep, send):
        other = flipped(send, "pole", 1)
        terms = [keep, other]
        for mask in masks:
            half = terms[0].shape[0] // 2
            out = sum(term[half:] for term in terms)
            terms = [term[:half] for term in terms] + [flipped(out, "pole", mask)]
        return sum(terms).reshape(count * order, width)

    own_y, own_z = [], []
    for c in range(chunks):
        keep_y, keep_z, send_y, send_z = second_solve(
            c, width, owners, pole_values, source, inverse, coupled, arrivals[c], added[c]
        )
        own_y.append(pole_sum(keep_y, send_y))
        own_z.append(pole_sum(keep_z, send_z))
    own_y = jnp.concatenate(own_y, axis=1)
    own_z = jnp.concatenate(own_z, axis=1)
    near = [("pole", i) for i in range(owners.bit_length() - 1)]
    near.insert(1, ("dom", 0))
    far = [("dom", i) for i in range(1, parts.bit_length() - 1)]
    gram = summed_everywhere(inner_products(own_y, own_y), near, far)
    projected = summed_everywhere(inner_products(own_y, own_z), near, far)
    row_total = blocks * order * parts
    basis, inverse_factor = orthonormalized(row_total, gram, own_y)
    rayleigh = congruence(row_total, inverse_factor, projected)
    return (basis.reshape(1, count, order, vectors), rayleigh)


def solution(mesh):
    in_specs = (
        P("dom", None, None, None),
        P("dom", None, None, None),
        P("pole", "dom", None, None, None, None),
        P("pole", "dom", None, None, None, None),
        P("pole", None),
    )
    out_specs = (P("dom", "pole", None, None), P())
    return jax.shard_map(
        on_device, mesh=mesh, in_specs=in_specs, out_specs=out_specs, check_vma=False
    )
```

```python
import functools
import jax
import jax.numpy as jnp
from jax import lax
from jax.experimental import pallas as pl
from jax.experimental.pallas import tpu as pltpu
from jax.sharding import PartitionSpec as P


F32 = jnp.float32
BF16 = jnp.bfloat16
LANES = 128
AHEAD = 3
STEP = 16
PIECES = 2
HIGHEST = lax.Precision.HIGHEST


def shifted(x, axis, by):
    length = lax.axis_size(axis)
    pairs = [(i, i + by) for i in range(length) if 0 <= i + by < length]
    return lax.ppermute(x, axis, pairs)


def flipped(x, axis, mask):
    return lax.ppermute(x, axis, [(i, i ^ mask) for i in range(lax.axis_size(axis))])


def complex_apply(stacked, vectors):
    order = stacked.shape[0] // 2
    width = vectors.shape[1] // 2
    out = jnp.dot(stacked, vectors.astype(BF16), preferred_element_type=F32)
    real = out[:order, :width] - out[order:, width:]
    imag = out[:order, width:] + out[order:, :width]
    return jnp.concatenate([real, imag], axis=1)


def real_apply(matrix, vectors):
    return jnp.dot(matrix, vectors.astype(BF16), preferred_element_type=F32)


def transposed_apply(matrix, vectors):
    return lax.dot_general(
        matrix, vectors.astype(BF16), (((0,), (0,)), ((), ())), preferred_element_type=F32
    )


def block_copies(k, f_hbm, g_hbm, u_hbm, fv, gv, uv, sem):
    return (
        pltpu.make_async_copy(f_hbm.at[k], fv.at[k], sem.at[0, k]),
        pltpu.make_async_copy(g_hbm.at[k], gv.at[k], sem.at[1, k]),
        pltpu.make_async_copy(u_hbm.at[k], uv.at[k], sem.at[2, k]),
    )


def fetch_ahead(blocks, copies, k):
    @pl.when(k + AHEAD < blocks)
    def _():
        for copy in copies(k + AHEAD):
            copy.start()


def first_kernel(groups, f_hbm, g_hbm, u_hbm, i_hbm, *refs):
    tops, sbs = refs[:groups], refs[groups : 2 * groups]
    fv, gv, uv, sv, ut, hold, sem, s_sem = refs[2 * groups :]
    blocks = gv.shape[0]
    order = uv.shape[1]
    width = fv.shape[2] // groups
    lanes = [slice(c * width, (c + 1) * width) for c in range(groups)]
    copies = functools.partial(
        block_copies, f_hbm=f_hbm, g_hbm=g_hbm, u_hbm=u_hbm, fv=fv, gv=gv, uv=uv, sem=sem
    )
    fetch = functools.partial(fetch_ahead, blocks, copies)
    for k in range(min(AHEAD, blocks)):
        for copy in copies(k):
            copy.start()
    s_copy = pltpu.make_async_copy(i_hbm.at[0], sv, s_sem)
    for copy in copies(0):
        copy.wait()
    for c in range(groups):
        out = jnp.dot(gv[0], fv[0, :, lanes[c]], preferred_element_type=F32)
        hold[c, 0] = jnp.concatenate([out[:order], out[order:]], axis=1)
    ut[0] = uv[0].T

    fetch(0)

    def forward(k, carry):
        fetch(k)
        for copy in copies(k):
            copy.wait()
        coupled = [real_apply(ut[(k + 1) % 2], hold[c, k - 1]) for c in range(groups)]
        for c in range(groups):
            given = fv[k, :, lanes[c]].astype(F32)
            hold[c, k] = complex_apply(
                gv[k], coupled[c] + jnp.concatenate([given, jnp.zeros_like(given)], axis=1)
            )
        ut[k % 2] = uv[k].T
        return carry

    s_copy.start()
    lax.fori_loop(1, blocks, forward, 0)
    s_copy.wait()
    for c in range(groups):
        sbs[c][...] = complex_apply(sv[...], hold[c, blocks - 1])

    def backward(i, carry):
        k = blocks - 2 - i
        coupled = [real_apply(uv[k], hold[c, k + 1]) for c in range(groups)]
        for c in range(groups):
            hold[c, k] = hold[c, k] + complex_apply(gv[k], coupled[c])
        return carry

    lax.fori_loop(0, blocks - 1, backward, 0)
    for c in range(groups):
        tops[c][...] = hold[c, 0]


def first_solve(groups, source, inverse, coupled, factors):
    blocks, stacked, order = inverse.shape
    vectors = source.shape[2]
    width = vectors // groups
    tip = jax.ShapeDtypeStruct((order, 2 * width), F32)
    hbm = pl.BlockSpec(memory_space=pl.ANY)
    vmem = pl.BlockSpec(memory_space=pltpu.VMEM)
    flops = 2 * order * order * 2 * vectors * (5 * blocks - 3)
    outs = pl.pallas_call(
        functools.partial(first_kernel, groups),
        out_shape=(tip,) * (2 * groups),
        in_specs=[hbm] * 4,
        out_specs=(vmem,) * (2 * groups),
        scratch_shapes=[
            pltpu.VMEM((blocks, order, vectors), BF16),
            pltpu.VMEM((blocks, stacked, order), BF16),
            pltpu.VMEM((blocks, order, order), BF16),
            pltpu.VMEM((stacked, order), BF16),
            pltpu.VMEM((2, order, order), BF16),
            pltpu.VMEM((groups, blocks, order, 2 * width), F32),
            pltpu.SemaphoreType.DMA((3, blocks)),
            pltpu.SemaphoreType.DMA,
        ],
        cost_estimate=pl.CostEstimate(flops=flops, transcendentals=0, bytes_accessed=14 * 2**20),
        name="first_solve",
    )(source, inverse, coupled, factors)
    return outs[:groups], outs[groups:]


def below_kernel(sb_hbm, next_hbm, i_hbm, u_hbm, below_ref, lifted_ref, sb, top_next, kv, uv, sem):
    copies = (
        pltpu.make_async_copy(next_hbm, top_next, sem.at[0]),
        pltpu.make_async_copy(i_hbm.at[1], kv, sem.at[1]),
        pltpu.make_async_copy(sb_hbm, sb, sem.at[2]),
        pltpu.make_async_copy(u_hbm.at[u_hbm.shape[0] - 1], uv, sem.at[3]),
    )
    for copy in copies:
        copy.start()
    copies[0].wait()
    copies[1].wait()
    product = complex_apply(kv[...], top_next[...])
    copies[2].wait()
    below = sb[...] - product
    below_ref[...] = below
    copies[3].wait()
    lifted_ref[...] = transposed_apply(uv[...], below)


def interface_below(s_times, top_next, factors, coupled):
    shape = jax.ShapeDtypeStruct(top_next.shape, F32)
    order, width = top_next.shape
    vmem = pl.BlockSpec(memory_space=pltpu.VMEM)
    hbm = pl.BlockSpec(memory_space=pl.ANY)
    return pl.pallas_call(
        below_kernel,
        out_shape=(shape, shape),
        in_specs=[hbm] * 4,
        out_specs=(vmem, vmem),
        scratch_shapes=[
            pltpu.VMEM(top_next.shape, F32),
            pltpu.VMEM(top_next.shape, F32),
            pltpu.VMEM((2 * order, order), BF16),
            pltpu.VMEM((order, order), BF16),
            pltpu.SemaphoreType.DMA((4,)),
        ],
        cost_estimate=pl.CostEstimate(
            flops=6 * order * order * width, transcendentals=0, bytes_accessed=4 * 2**20
        ),
        name="interface_below",
    )(s_times, top_next, factors, coupled)


def above_kernel(parts, below_hbm, next_hbm, i_hbm, u_hbm, added_ref, below, top_next, wv, uv, sem):
    copies = (
        pltpu.make_async_copy(below_hbm, below, sem.at[0]),
        pltpu.make_async_copy(i_hbm.at[2], wv, sem.at[1]),
        pltpu.make_async_copy(next_hbm, top_next, sem.at[2]),
        pltpu.make_async_copy(u_hbm.at[u_hbm.shape[0] - 1], uv, sem.at[3]),
    )
    for copy in copies:
        copy.start()
    for copy in copies[:3]:
        copy.wait()
    above = top_next[...] - complex_apply(wv[...], below[...])
    topmost = lax.axis_index("dom") == parts - 1
    above = jnp.where(topmost, jnp.zeros_like(above), above)
    copies[3].wait()
    added_ref[...] = real_apply(uv[...], above)


def interface_above(parts, below, top_next, factors, coupled):
    order, width = top_next.shape
    vmem = pl.BlockSpec(memory_space=pltpu.VMEM)
    hbm = pl.BlockSpec(memory_space=pl.ANY)
    return pl.pallas_call(
        functools.partial(above_kernel, parts),
        out_shape=jax.ShapeDtypeStruct(top_next.shape, F32),
        in_specs=[hbm] * 4,
        out_specs=vmem,
        scratch_shapes=[
            pltpu.VMEM(top_next.shape, F32),
            pltpu.VMEM(top_next.shape, F32),
            pltpu.VMEM((2 * order, order), BF16),
            pltpu.VMEM((order, order), BF16),
            pltpu.SemaphoreType.DMA((4,)),
        ],
        cost_estimate=pl.CostEstimate(
            flops=6 * order * order * width, transcendentals=0, bytes_accessed=4 * 2**20
        ),
        name="interface_above",
    )(below, top_next, factors, coupled)


def second_kernel(
    lane, owners, pole_ref, f_hbm, g_hbm, u_hbm, arrive_hbm, added_hbm,
    keep_y, keep_z, send_y, send_z, fv, gv, uv, ut, hold, yv, zv, arrive, added, sem, out_sem, tip_sem,
):
    blocks = gv.shape[0]
    count = blocks // owners
    width = fv.shape[2]
    copies = functools.partial(
        block_copies, f_hbm=f_hbm.at[:, :, pl.ds(lane, width)], g_hbm=g_hbm, u_hbm=u_hbm,
        fv=fv, gv=gv, uv=uv, sem=sem,
    )
    fetch = functools.partial(fetch_ahead, blocks, copies)
    for k in range(min(AHEAD, blocks)):
        for copy in copies(k):
            copy.start()

    arrive_copy = pltpu.make_async_copy(arrive_hbm, arrive, tip_sem.at[0])
    added_copy = pltpu.make_async_copy(added_hbm, added, tip_sem.at[1])
    arrive_copy.start()

    def given(k):
        real = fv[k].astype(F32)
        return jnp.concatenate([real, jnp.zeros_like(real)], axis=1)

    for copy in copies(0):
        copy.wait()
    arrive_copy.wait()
    hold[0] = complex_apply(gv[0], given(0) + arrive[...])
    added_copy.start()
    ut[0] = uv[0].T

    fetch(0)

    def forward(k, carry):
        fetch(k)
        for copy in copies(k):
            copy.wait()
        coupled = real_apply(ut[(k + 1) % 2], hold[k - 1])
        hold[k] = complex_apply(gv[k], given(k) + coupled)
        ut[k % 2] = uv[k].T
        return carry

    lax.fori_loop(1, blocks - 1, forward, 0)
    last = blocks - 1
    for copy in copies(last):
        copy.wait()
    added_copy.wait()
    coupled = real_apply(ut[(last + 1) % 2], hold[last - 1])
    hold[last] = complex_apply(gv[last], (given(last) + added[...]) + coupled)

    zr, zi, wr, wi = (pole_ref[0, i] for i in range(4))
    zwr = wr * zr - wi * zi
    zwi = wr * zi + wi * zr
    pole = lax.axis_index("pole")
    low = pole % 2
    high = pole // 2

    def emit(k, x):
        real, imag = x[:, :width], x[:, width:]
        y = wr * real - wi * imag
        z = zwr * real - zwi * imag - wr * fv[k].astype(F32)
        owner = k // count
        slot = ((owner // 2) ^ high) * count + k % count

        yv[k] = y
        zv[k] = z

        @pl.when(owner % 2 == low)
        def _():
            pltpu.make_async_copy(yv.at[k], keep_y.at[slot], out_sem.at[0, k]).start()
            pltpu.make_async_copy(zv.at[k], keep_z.at[slot], out_sem.at[1, k]).start()

        @pl.when(owner % 2 != low)
        def _():
            pltpu.make_async_copy(yv.at[k], send_y.at[slot], out_sem.at[0, k]).start()
            pltpu.make_async_copy(zv.at[k], send_z.at[slot], out_sem.at[1, k]).start()

    emit(last, hold[last])

    def backward(i, carry):
        k = blocks - 2 - i
        x = hold[k] + complex_apply(gv[k], real_apply(uv[k], hold[k + 1]))
        hold[k] = x
        emit(k, x)
        return carry

    lax.fori_loop(0, blocks - 1, backward, 0)
    for k in range(blocks):
        pltpu.make_async_copy(yv.at[k], keep_y.at[0], out_sem.at[0, k]).wait()
        pltpu.make_async_copy(zv.at[k], keep_z.at[0], out_sem.at[1, k]).wait()


def second_solve(chunk, width, owners, pole_values, source, inverse, coupled, arriving, added):
    blocks, stacked, order = inverse.shape
    part = jax.ShapeDtypeStruct((blocks // 2, order, width), F32)
    hbm = pl.BlockSpec(memory_space=pl.ANY)
    vmem = pl.BlockSpec(memory_space=pltpu.VMEM)
    smem = pl.BlockSpec(memory_space=pltpu.SMEM)
    flops = 2 * order * order * 2 * width * (5 * blocks - 3)
    return pl.pallas_call(
        functools.partial(second_kernel, chunk * width, owners),
        out_shape=(part,) * 4,
        in_specs=[smem] + [hbm] * 5,
        out_specs=(hbm,) * 4,
        scratch_shapes=[
            pltpu.VMEM((blocks, order, width), BF16),
            pltpu.VMEM((blocks, stacked, order), BF16),
            pltpu.VMEM((blocks, order, order), BF16),
            pltpu.VMEM((2, order, order), BF16),
            pltpu.VMEM((blocks, order, 2 * width), F32),
            pltpu.VMEM((blocks, order, width), F32),
            pltpu.VMEM((blocks, order, width), F32),
            pltpu.VMEM((order, 2 * width), F32),
            pltpu.VMEM((order, 2 * width), F32),
            pltpu.SemaphoreType.DMA((3, blocks)),
            pltpu.SemaphoreType.DMA((2, blocks)),
            pltpu.SemaphoreType.DMA((2,)),
        ],
        cost_estimate=pl.CostEstimate(flops=flops, transcendentals=0, bytes_accessed=16 * 2**20),
        name="second_solve",
    )(pole_values, source, inverse, coupled, arriving, added)


def panel_kernel(total, start, stop, in_ref, acc):
    n = acc.shape[0]
    if start == 0:
        rows = lax.broadcasted_iota(jnp.int32, (n, n), 0)
        cols = lax.broadcasted_iota(jnp.int32, (n, n), 1)
        acc[:, :n] = in_ref[...] / total
        acc[:, n:] = (rows == cols).astype(F32)
    else:
        acc[...] = in_ref[...]
    lane = min(LANES, n)
    row = lax.broadcasted_iota(jnp.int32, (STEP, lane), 0)

    def spread(x):
        return jnp.broadcast_to(x, (STEP, lane))

    for r in range(start, stop, STEP):
        low = r // lane * lane
        high = (r + STEP + lane - 1) // lane * lane
        panel = acc[r : r + STEP, low : n + high]
        tiles = [panel[:, i : i + lane] for i in range(0, panel.shape[1], lane)]
        columns = [spread(panel[:, r - low + j : r - low + j + 1]) for j in range(STEP)]
        scale = jnp.ones((STEP, lane), F32)
        for k in range(STEP):
            inv = lax.rsqrt(spread(columns[k][k : k + 1]))
            scale = jnp.where(row == k, inv, scale)
            m = jnp.where(row > k, columns[k], 0.0) * (inv * inv)
            for j in range(k + 1, STEP):
                columns[j] = columns[j] - m * spread(columns[j][k : k + 1])
            tiles = [t - m * spread(t[k : k + 1]) for t in tiles]
        done = jnp.concatenate([t * scale for t in tiles], axis=1)
        acc[r : r + STEP, low : n + high] = done
        if r + STEP < n:
            left = done[:, : n - low].T[r + STEP - low :]
            acc[r + STEP :, low : n + high] -= jnp.dot(
                left, done, precision=HIGHEST, preferred_element_type=F32
            )


def basis_kernel(acc_ref, y_ref, basis_ref, inverse_ref):
    n = acc_ref.shape[0]
    rows = lax.broadcasted_iota(jnp.int32, (n, n), 0)
    cols = lax.broadcasted_iota(jnp.int32, (n, n), 1)
    inverse = jnp.where(cols <= rows, acc_ref[:, n:], 0.0)
    inverse_ref[...] = inverse
    basis_ref[...] = lax.dot_general(
        y_ref[...], inverse, (((1,), (1,)), ((), ())),
        precision=HIGHEST, preferred_element_type=F32,
    )


def congruence_kernel(total, inverse_ref, proj_ref, ray_ref):
    inverse = inverse_ref[...]
    middle = jnp.dot(
        inverse, proj_ref[...] / total, precision=HIGHEST, preferred_element_type=F32
    )
    ray_ref[...] = lax.dot_general(
        middle, inverse, (((1,), (1,)), ((), ())), precision=HIGHEST, preferred_element_type=F32
    )


def congruence(total, inverse, projected):
    vmem = pl.BlockSpec(memory_space=pltpu.VMEM)
    return pl.pallas_call(
        functools.partial(congruence_kernel, float(total)),
        out_shape=jax.ShapeDtypeStruct(inverse.shape, F32),
        in_specs=[vmem] * 2,
        out_specs=vmem,
        cost_estimate=pl.CostEstimate(flops=2**30, transcendentals=0, bytes_accessed=2**20),
        name="congruence",
    )(inverse, projected)


def orthonormalized(total, gram, y):
    n = gram.shape[0]
    vmem = pl.BlockSpec(memory_space=pltpu.VMEM)
    rows = n // PIECES
    acc = gram
    for p in range(PIECES):
        acc = pl.pallas_call(
            functools.partial(panel_kernel, float(total), p * rows, (p + 1) * rows),
            out_shape=jax.ShapeDtypeStruct((n, 2 * n), F32),
            in_specs=[vmem],
            out_specs=vmem,
            cost_estimate=pl.CostEstimate(
                flops=2**31, transcendentals=0, bytes_accessed=2**20
            ),
            name="factor_panels",
        )(acc)
    return pl.pallas_call(
        basis_kernel,
        out_shape=(jax.ShapeDtypeStruct(y.shape, F32), jax.ShapeDtypeStruct((n, n), F32)),
        in_specs=[vmem] * 2,
        out_specs=(vmem, vmem),
        cost_estimate=pl.CostEstimate(
            flops=2**31, transcendentals=0, bytes_accessed=3 * 2**20
        ),
        name="basis",
    )(acc, y)


def inner_products(left, right_side):
    return lax.dot_general(
        left,
        right_side,
        (((0,), (0,)), ((), ())),
        precision=lax.Precision.HIGHEST,
        preferred_element_type=F32,
    )


def summed_everywhere(x, near, far):
    kept = []
    for axis, i in near:
        half = x.shape[0] // 2
        upper = (lax.axis_index(axis) >> i) & 1 == 1
        mine = jnp.where(upper, x[half:], x[:half])
        other = jnp.where(upper, x[:half], x[half:])
        x = mine + flipped(other, axis, 1 << i)
        kept.append(upper)
    axis, masks = far
    x = x + sum(flipped(x, axis, mask) for mask in masks)
    for (axis, i), upper in zip(reversed(near), reversed(kept)):
        other = flipped(x, axis, 1 << i)
        x = jnp.where(upper, jnp.concatenate([other, x]), jnp.concatenate([x, other]))
    return x


def on_device(initial_block, coupling, pivots, interface, pole_values):
    blocks = coupling.shape[1]
    order = coupling.shape[2]
    vectors = initial_block.shape[3]
    width = min(LANES, vectors)
    owners = lax.axis_size("pole")
    parts = lax.axis_size("dom")
    count = blocks // owners
    source = initial_block[0]
    coupled = coupling[0]
    inverse = pivots[0, 0].reshape(blocks, 2 * order, order)
    factors = interface[0, 0].reshape(3, 2 * order, order)
    chunks = vectors // width
    tips, s_times = first_solve(chunks, source, inverse, coupled, factors)
    tops, belows, arrivals, added = [], [], [], []
    for c in range(chunks):
        tops.append(shifted(tips[c], "dom", -1))
    for c in range(chunks):
        belows.append(interface_below(s_times[c], tops[c], factors, coupled))
        arrivals.append(shifted(belows[c][1], "dom", 1))
        added.append(interface_above(parts, belows[c][0], tops[c], factors, coupled))
    masks = [1 << i for i in range(1, owners.bit_length() - 1)]

    def pole_sum(keep, send):
        other = flipped(send, "pole", 1)
        terms = [keep, other]
        for mask in masks:
            half = terms[0].shape[0] // 2
            out = sum(term[half:] for term in terms)
            terms = [term[:half] for term in terms] + [flipped(out, "pole", mask)]
        return sum(terms).reshape(count * order, width)

    own_y, own_z = [], []
    for c in range(chunks):
        keep_y, keep_z, send_y, send_z = second_solve(
            c, width, owners, pole_values, source, inverse, coupled, arrivals[c], added[c]
        )
        own_y.append(pole_sum(keep_y, send_y))
        own_z.append(pole_sum(keep_z, send_z))
    own_y = jnp.concatenate(own_y, axis=1)
    own_z = jnp.concatenate(own_z, axis=1)
    near = [("pole", i) for i in range(owners.bit_length() - 1)]
    near.insert(1, ("dom", 0))
    far = ("dom", tuple(range(2, parts, 2)))
    gram = summed_everywhere(inner_products(own_y, own_y), near, far)
    projected = summed_everywhere(inner_products(own_y, own_z), near, far)
    row_total = blocks * order * parts
    basis, inverse_factor = orthonormalized(row_total, gram, own_y)
    rayleigh = congruence(row_total, inverse_factor, projected)
    return (basis.reshape(1, count, order, vectors), rayleigh)


def solution(mesh):
    in_specs = (
        P("dom", None, None, None),
        P("dom", None, None, None),
        P("pole", "dom", None, None, None, None),
        P("pole", "dom", None, None, None, None),
        P("pole", None),
    )
    out_specs = (P("dom", "pole", None, None), P())
    return jax.shard_map(
        on_device, mesh=mesh, in_specs=in_specs, out_specs=out_specs, check_vma=False
    )
```
